32 devices in a mesh: dp: 2 (over x), sp: 16 (over y, z, core).
Axes of the slice: x: 2, y: 2, z: 4, core: 2. Of those that a mesh axis runs over, the one named last changes fastest.
Arguments:
- q: bfloat16 [64, 32, 64], P('dp'), parts along dimension 0
- k: bfloat16 [64, 8192, 8, 64], P('dp', 'sp'), parts along dimension 0
- v: bfloat16 [64, 8192, 8, 64], P('dp', 'sp'), parts along dimension 0
Outputs:
- q: bfloat16 [64, 32, 64], P('dp'), parts along dimension 0
There are 2 independent parts. The reference program is written for one: setup_inputs(seed, part) draws one part's arguments, and reference() takes and returns one part's arrays. A program takes and returns all parts, laid end to end along the dimension named above; each array names one.
All inputs are finite; a program needn't handle non-finite values.
Results may differ from the reference program's by a relative error of at most 0.012.
Values are sent between devices in bfloat16 or wider.
A program may use at most 2 GiB of HBM per device.

```python
import jax
import jax.numpy as jnp

BATCH = 32
CACHE = 8192
HEADS = 32
KV_HEADS = 8
HEAD = 64


def setup_inputs(seed: int = 0, part: int = 0) -> dict:
    kq, kk, kv = (jax.random.fold_in(k, part) for k in jax.random.split(jax.random.key(seed), 3))
    return {
        "q": (3 * jax.random.normal(kq, (BATCH, HEADS, HEAD), jnp.float32)).astype(jnp.bfloat16),
        "k": jax.random.normal(kk, (BATCH, CACHE, KV_HEADS, HEAD), jnp.float32).astype(jnp.bfloat16),
        "v": jax.random.normal(kv, (BATCH, CACHE, KV_HEADS, HEAD), jnp.float32).astype(jnp.bfloat16),
    }


def einsum(form, a, b):
    return jnp.einsum(form, a.astype(jnp.float32), b.astype(jnp.float32))


def reference(q, k, v):
    grouped = q.reshape(BATCH, KV_HEADS, -1, HEAD)
    scores = einsum("bgsd,bugd->bgsu", grouped, k) * HEAD**-0.5
    weights = jax.nn.softmax(scores, -1).astype(jnp.bfloat16)
    return einsum("bgsu,bugd->bgsd", weights, v).astype(jnp.bfloat16).reshape(BATCH, HEADS, HEAD)
```

```python
import jax
import jax.numpy as jnp
from jax import lax
from jax.experimental import pallas as pl
from jax.experimental.pallas import tpu as pltpu
from jax.sharding import PartitionSpec as P

MESH = pl.DeviceIdType.MESH
N = 16
G = 8
S = 4
LAG = 3


def owner_of(g, quarter):
    turn = lax.rem(g, 4)
    inner, core = turn // 2, lax.rem(turn, 2)
    y, side = quarter // 2, quarter % 2
    z = inner * (1 + side) + (1 - inner) * 3 * side
    return (y * 4 + z) * 2 + core


def place_of(me):
    y, z, core = me // 8, lax.rem(me, 8) // 2, lax.rem(me, 2)
    inner = jnp.where((z == 1) | (z == 2), 1, 0)
    side = z // 2
    return inner * 2 + core, y * 2 + side


def kernel(q_hbm, k_hbm, v_hbm, o_ref, q_s, k_s, v_s, w_s, part_s, stat_s, got_p, got_s, q_sem, k_sem, v_sem, send_p, send_t, send_o, recv_p, recv_t, recv_o):
    me = lax.axis_index("sp")
    turn, quarter = place_of(me)

    def kcopy(g):
        return pltpu.make_async_copy(k_hbm.at[pl.ds(g * S, S)], k_s.at[pl.ds(g * S, S)], k_sem.at[g])

    def vcopy(g):
        return pltpu.make_async_copy(v_hbm.at[pl.ds(g * S, S)], v_s.at[pl.ds(g * S, S)], v_sem.at[g])

    qc = pltpu.make_async_copy(q_hbm, q_s, q_sem)
    qc.start()
    kcopy(0).start(priority=1)
    kcopy(1).start(priority=1)
    for g in range(G - 2):
        vcopy(g).start(priority=1)
        kcopy(g + 2).start(priority=1)
    vcopy(G - 2).start(priority=1)
    vcopy(G - 1).start(priority=1)

    barrier = pltpu.get_barrier_semaphore()
    for d in range(1, N):
        pl.semaphore_signal(barrier, inc=1, device_id={"sp": lax.rem(me + d, N)}, device_id_type=MESH)

    lane64 = lax.broadcasted_iota(jnp.int32, (16, 128), 1) // 64
    row4 = lax.broadcasted_iota(jnp.int32, (16, 128), 0) // 4
    lane = lax.broadcasted_iota(jnp.int32, (64, 128), 1) // 4
    rowid = lax.broadcasted_iota(jnp.int32, (16, 128), 0)
    laneid = lax.broadcasted_iota(jnp.int32, (16, 128), 1)

    def scores(g):
        slot = lax.rem(g, 2)
        mrow = jnp.zeros((16, 128), jnp.float32)
        lrow = jnp.zeros((16, 128), jnp.float32)
        for i in range(S):
            qb = q_s[g * S + i].astype(jnp.float32)
            qq = jnp.concatenate([qb, qb], -1)
            for t in range(2):
                piece = qq[16 * t:16 * t + 16]
                lo = jnp.where(row4 == lane64, piece, 0.0)
                hi = jnp.where(row4 == lane64 + 2, piece, 0.0)
                lhs = jnp.concatenate([lo, hi], -1).astype(jnp.bfloat16)
                s = jnp.dot(lhs, k_s[g * S + i, 256 * t:256 * t + 256, :], preferred_element_type=jnp.float32)
                m = jnp.max(s, -1, keepdims=True)
                p = jnp.exp((s - m) * 0.125)
                l = jnp.sum(p, -1, keepdims=True)
                r = 32 * i + 16 * t
                w_s[slot, r:r + 16, :] = p.astype(jnp.bfloat16)
                hit = laneid == rowid + r
                mrow = jnp.where(hit, m * 0.125, mrow)
                lrow = jnp.where(hit, l, lrow)
        stat_s[g, 0:1] = jnp.sum(mrow, 0, keepdims=True)
        stat_s[g, 1:2] = jnp.sum(lrow, 0, keepdims=True)

    def values(g):
        w = w_s[lax.rem(g, 2)]
        acc = jnp.zeros((64, 128), jnp.float32)
        for i in range(S):
            res = lax.dot_general(v_s[g * S + i], w, (((1,), (1,)), ((), ())), preferred_element_type=jnp.float32)
            for h in range(8):
                acc = jnp.where(lane == i * 8 + h, res[64 * h:64 * h + 64], acc)
        part_s[g] = acc.astype(jnp.bfloat16).reshape(4, 16, 128)

    def give(g):
        turns = g // 4
        for c in range(4):
            to = owner_of(g, c)

            @pl.when(to != me)
            def _():
                pltpu.make_async_remote_copy(
                    src_ref=part_s.at[g, c], dst_ref=got_p.at[turns, me], send_sem=send_p.at[turns], recv_sem=recv_p.at[turns],
                    device_id={"sp": to}, device_id_type=MESH).start()
                pltpu.make_async_remote_copy(
                    src_ref=stat_s.at[g], dst_ref=got_s.at[turns, me], send_sem=send_t.at[turns], recv_sem=recv_t.at[turns],
                    device_id={"sp": to}, device_id_type=MESH).start()

            @pl.when(to == me)
            def _():
                got_p[turns, me] = part_s[g, c]
                got_s[turns, me] = stat_s[g]

    def all_p(r, send, recv):
        return pltpu.make_async_remote_copy(
            src_ref=got_p.at[r, pl.ds(0, N - 1)], dst_ref=got_p.at[r, pl.ds(0, N - 1)], send_sem=send.at[r], recv_sem=recv.at[r],
            device_id={"sp": me}, device_id_type=MESH)

    def all_t(r):
        return pltpu.make_async_remote_copy(
            src_ref=got_s.at[r, pl.ds(0, N - 1)], dst_ref=got_s.at[r, pl.ds(0, N - 1)], send_sem=send_t.at[r], recv_sem=recv_t.at[r],
            device_id={"sp": me}, device_id_type=MESH)

    def together(r):
        all_p(r, send_p, recv_p).wait_recv()
        all_t(r).wait_recv()
        stats = got_s[r]
        highs = [stats[j, 0:1] for j in range(N)]
        high = highs[0]
        for h in highs[1:]:
            high = jnp.maximum(high, h)
        seen = jnp.zeros((16, 128), jnp.float32)
        total = jnp.zeros((1, 128), jnp.float32)
        for j in range(N):
            scale = jnp.exp(highs[j] - high)
            seen = seen + got_p[r, j].astype(jnp.float32) * scale
            total = total + stats[j, 1:2] * scale
        g = r * 4 + turn
        o_ref[g, quarter] = (seen / total).astype(jnp.bfloat16)
        for d in range(1, N):
            pltpu.make_async_remote_copy(
                src_ref=o_ref.at[g, quarter], dst_ref=o_ref.at[g, quarter], send_sem=send_o.at[r], recv_sem=recv_o.at[r],
                device_id={"sp": lax.rem(me + d, N)}, device_id_type=MESH).start()

    qc.wait()
    kcopy(0).wait()
    scores(0)
    pl.semaphore_wait(barrier, N - 1)

    def body(g, _):
        kcopy(g + 1).wait()
        vcopy(g).wait()
        values(g)
        scores(g + 1)
        give(g)

        @pl.when(g == turn + LAG)
        def _():
            together(0)

        return 0

    lax.fori_loop(0, G - 1, body, 0)
    vcopy(G - 1).wait()
    values(G - 1)
    give(G - 1)
    together(1)
    for r in range(2):
        all_p(r, send_p, recv_p).wait_send()
        all_t(r).wait_send()
        all_p(r, send_o, recv_o).wait_send()
        all_p(r, send_o, recv_o).wait_recv()


def solution(mesh):
    def step(q, k, v):
        k = jnp.transpose(k, (0, 2, 3, 1)).reshape(32, 512, 512)
        v = jnp.transpose(v, (0, 2, 3, 1)).reshape(32, 512, 512)
        o = pl.pallas_call(
            kernel,
            out_shape=pltpu.VMEM((G, 4, 16, 128), jnp.bfloat16),
            in_specs=[pl.BlockSpec(memory_space=pl.ANY)] * 3,
            out_specs=pl.BlockSpec(memory_space=pltpu.VMEM),
            scratch_shapes=[
                pltpu.VMEM((32, 32, 64), jnp.bfloat16),
                pltpu.VMEM((32, 512, 512), jnp.bfloat16),
                pltpu.VMEM((32, 512, 512), jnp.bfloat16),
                pltpu.VMEM((2, 128, 512), jnp.bfloat16),
                pltpu.VMEM((G, 4, 16, 128), jnp.bfloat16),
                pltpu.VMEM((G, 2, 128), jnp.float32),
                pltpu.VMEM((2, N, 16, 128), jnp.bfloat16),
                pltpu.VMEM((2, N, 2, 128), jnp.float32),
                pltpu.SemaphoreType.DMA(()),
                pltpu.SemaphoreType.DMA((G,)),
                pltpu.SemaphoreType.DMA((G,)),
            ] + [pltpu.SemaphoreType.DMA((2,))] * 6,
            compiler_params=pltpu.CompilerParams(vmem_limit_bytes=56 << 20, collective_id=0, has_side_effects=True),
        )(q, k, v)
        return o.reshape(G, 64, 128).transpose(0, 2, 1).reshape(32, 32, 64)

    return jax.shard_map(
        step,
        mesh=mesh,
        in_specs=(P("dp", None, None), P("dp", "sp", None, None), P("dp", "sp", None, None)),
        out_specs=P("dp", None, None),
        check_vma=False,
    )
```

```python
import jax
import jax.numpy as jnp
from jax import lax
from jax.experimental import pallas as pl
from jax.experimental.pallas import tpu as pltpu
from jax.sharding import PartitionSpec as P

MESH = pl.DeviceIdType.MESH
F32, BF16 = jnp.float32, jnp.bfloat16
N = 16
G = 8
S = 4
A = 1


def owner_of(g, quarter):
    core, outer = g // 4, g // 2 % 2
    y, side = quarter // 2, quarter % 2
    z = 3 * side if outer else 1 + side
    return (y * 4 + z) * 2 + core


def place_of(me):
    y, z, core = me // 8, lax.rem(me, 8) // 2, lax.rem(me, 2)
    inner = (z == 1) | (z == 2)
    return core * 4 + jnp.where(inner, 0, 2), y * 2 + z // 2, inner


def kernel(q_hbm, k_hbm, v_hbm, o_ref, q_s, k_s, v_s, w0_s, w1_s, part_s, stat_s, got_p, got_s, q_sem, k_sem, v_sem, send_p, send_t, send_o, recv_p, recv_t, recv_o):
    me = lax.axis_index("sp")
    first, quarter, inner = place_of(me)
    w_s = (w0_s, w1_s)

    def give(g):
        r = g % 2
        for c in range(4):
            to = owner_of(g, c)

            @pl.when(me != to)
            def _():
                pltpu.make_async_remote_copy(
                    src_ref=part_s.at[g, c], dst_ref=got_p.at[r, me], send_sem=send_p, recv_sem=recv_p.at[r],
                    device_id={"sp": to}, device_id_type=MESH).start()
                pltpu.make_async_remote_copy(
                    src_ref=stat_s.at[g], dst_ref=got_s.at[r, me], send_sem=send_t, recv_sem=recv_t.at[r],
                    device_id={"sp": to}, device_id_type=MESH).start()

    def whole(ref, send, recv):
        return pltpu.make_async_remote_copy(src_ref=ref, dst_ref=ref, send_sem=send, recv_sem=recv, device_id={"sp": me}, device_id_type=MESH)

    def together(r):
        g = first + r
        whole(got_s.at[r, pl.ds(0, N - 1)], send_t, recv_t.at[r]).wait_recv()
        whole(got_p.at[r, pl.ds(0, N - 1)], send_p, recv_p.at[r]).wait_recv()
        got_p[r, me] = part_s[g, quarter]
        got_s[r, me] = stat_s[g]
        stats = got_s[r]
        highs = [stats[j, 0:1] for j in range(N)]
        high = highs[0]
        for h in highs[1:]:
            high = jnp.maximum(high, h)
        seen = jnp.zeros((16, 128), F32)
        total = jnp.zeros((1, 128), F32)
        for j in range(N):
            scale = jnp.exp(highs[j] - high)
            seen = seen + got_p[r, j].astype(F32) * scale
            total = total + stats[j, 1:2] * scale
        o_ref[g, quarter] = (seen / total).astype(BF16)
        for d in range(N - 1):
            to = d + jnp.where(d >= me, 1, 0)
            pltpu.make_async_remote_copy(
                src_ref=o_ref.at[g, quarter], dst_ref=o_ref.at[g, quarter], send_sem=send_o, recv_sem=recv_o,
                device_id={"sp": to}, device_id_type=MESH).start()

    def attend(q_sem, k_sem, v_sem):
        def kcopy(g):
            return pltpu.make_async_copy(k_hbm.at[pl.ds(g * S, S)], k_s.at[pl.ds(g * S, S)], k_sem.at[g])

        def vcopy(g):
            return pltpu.make_async_copy(v_hbm.at[pl.ds(g * S, S)], v_s.at[pl.ds(g * S, S)], v_sem.at[g])

        pltpu.make_async_copy(q_hbm, q_s, q_sem).start()
        kcopy(0).start(priority=1)

        def issue_k(j, _):
            kcopy(j).start(priority=1)
            return 0

        def issue(g, _):
            vcopy(g).start(priority=1)

            @pl.when(g + A + 1 < G)
            def _():
                kcopy(g + A + 1).start(priority=1)

            return 0

        lax.fori_loop(1, A + 1, issue_k, 0)
        lax.fori_loop(0, G, issue, 0)

        barrier = pltpu.get_barrier_semaphore()
        for d in range(1, N):
            pl.semaphore_signal(barrier, inc=1, device_id={"sp": lax.rem(me + d, N)}, device_id_type=MESH)

        lane64 = lax.broadcasted_iota(jnp.int32, (16, 128), 1) // 64
        row4 = lax.broadcasted_iota(jnp.int32, (16, 128), 0) // 4
        lane = lax.broadcasted_iota(jnp.int32, (64, 128), 1) // 4
        rowid = lax.broadcasted_iota(jnp.int32, (16, 128), 0)
        laneid = lax.broadcasted_iota(jnp.int32, (16, 128), 1)

        def scores(g):
            slot = g % 2
            mrow = jnp.zeros((16, 128), F32)
            lrow = jnp.zeros((16, 128), F32)
            for i in range(S):
                qb = q_s[g * S + i].astype(F32)
                qq = jnp.concatenate([qb, qb], -1)
                for t in range(2):
                    piece = qq[16 * t:16 * t + 16]
                    lo = jnp.where(row4 == lane64, piece, 0.0)
                    hi = jnp.where(row4 == lane64 + 2, piece, 0.0)
                    lhs = jnp.concatenate([lo, hi], -1).astype(BF16)
                    s = jnp.dot(lhs, k_s[g * S + i, 256 * t:256 * t + 256, :], preferred_element_type=F32)
                    m = jnp.max(s, -1, keepdims=True)
                    p = jnp.exp((s - m) * 0.125)
                    l = jnp.sum(p, -1, keepdims=True)
                    r = 32 * i + 16 * t
                    w_s[slot][r:r + 16, :] = p.astype(BF16)
                    hit = laneid == rowid + r
                    mrow = jnp.where(hit, m * 0.125, mrow)
                    lrow = jnp.where(hit, l, lrow)
            stat_s[g, 0:1] = jnp.sum(mrow, 0, keepdims=True)
            stat_s[g, 1:2] = jnp.sum(lrow, 0, keepdims=True)

        def values(g):
            w = w_s[g % 2][...]
            acc = jnp.zeros((64, 128), F32)
            for i in range(S):
                res = lax.dot_general(v_s[g * S + i], w, (((1,), (1,)), ((), ())), preferred_element_type=F32)
                for h in range(8):
                    acc = jnp.where(lane == i * 8 + h, res[64 * h:64 * h + 64], acc)
            return acc

        def finish(g, acc):
            part_s[g] = acc.astype(BF16).reshape(4, 16, 128)

        pltpu.make_async_copy(q_hbm, q_s, q_sem).wait()
        kcopy(0).wait()
        scores(0)
        for g in range(G):
            if g + 1 < G:
                kcopy(g + 1).wait()
            vcopy(g).wait()
            if g + 1 < G:
                scores(g + 1)
            finish(g, values(g))
            if g == 0:
                @pl.when(me >= 2)
                def _():
                    pl.semaphore_wait(barrier, N - 1)

            if g == 2:
                @pl.when(me < 2)
                def _():
                    pl.semaphore_wait(barrier, N - 1)
                    give(0)
                    give(1)

            if g < 2:
                @pl.when(me >= 2)
                def _():
                    give(g)
            else:
                give(g)
            if g == 5:
                @pl.when(inner & (first == 0))
                def _():
                    together(0)
                    together(1)

    attend(q_sem, k_sem, v_sem)

    @pl.when(jnp.logical_not(inner & (first == 0)))
    def _():
        together(0)
        together(1)

    sent = whole(got_p.at[:, pl.ds(0, N - 1)], send_p, recv_o)
    sent.wait_send()
    whole(got_s.at[:, pl.ds(0, N - 1)], send_t, recv_o).wait_send()
    whole(got_p.at[:, pl.ds(0, N - 1)], send_o, recv_o).wait_send()
    sent.wait_recv()


def solution(mesh):
    def step(q, k, v):
        k = jnp.transpose(k, (0, 2, 3, 1)).reshape(32, 512, 512)
        v = jnp.transpose(v, (0, 2, 3, 1)).reshape(32, 512, 512)
        o = pl.pallas_call(
            kernel,
            out_shape=pltpu.VMEM((G, 4, 16, 128), BF16),
            in_specs=[pl.BlockSpec(memory_space=pl.ANY)] * 3,
            out_specs=pl.BlockSpec(memory_space=pltpu.VMEM),
            scratch_shapes=[
                pltpu.VMEM((32, 32, 64), BF16),
                pltpu.VMEM((32, 512, 512), BF16),
                pltpu.VMEM((32, 512, 512), BF16),
                pltpu.VMEM((128, 512), BF16),
                pltpu.VMEM((128, 512), BF16),
                pltpu.VMEM((G, 4, 16, 128), BF16),
                pltpu.VMEM((G, 2, 128), F32),
                pltpu.VMEM((2, N, 16, 128), BF16),
                pltpu.VMEM((2, N, 2, 128), F32),
                pltpu.SemaphoreType.DMA(()),
                pltpu.SemaphoreType.DMA((G,)),
                pltpu.SemaphoreType.DMA((G,)),
                pltpu.SemaphoreType.DMA(()),
                pltpu.SemaphoreType.DMA(()),
                pltpu.SemaphoreType.DMA(()),
                pltpu.SemaphoreType.DMA((2,)),
                pltpu.SemaphoreType.DMA((2,)),
                pltpu.SemaphoreType.DMA(()),
            ],
            compiler_params=pltpu.CompilerParams(vmem_limit_bytes=56 << 20, collective_id=0, has_side_effects=True),
        )(q, k, v)
        return o.reshape(G, 64, 128).transpose(0, 2, 1).reshape(32, 32, 64)

    return jax.shard_map(
        step,
        mesh=mesh,
        in_specs=(P("dp", None, None), P("dp", "sp", None, None), P("dp", "sp", None, None)),
        out_specs=P("dp", None, None),
        check_vma=False,
    )
```

```python
import jax
import jax.numpy as jnp
from jax import lax
from jax.experimental import pallas as pl
from jax.experimental.pallas import tpu as pltpu
from jax.sharding import PartitionSpec as P

MESH = pl.DeviceIdType.MESH
F32, BF16 = jnp.float32, jnp.bfloat16
N = 16
G = 8
S = 4
A = 1


def owner_of(g, quarter):
    core, outer = g // 4, g // 2 % 2
    y, side = quarter // 2, quarter % 2
    z = 3 * side if outer else 1 + side
    return (y * 4 + z) * 2 + core


def place_of(me):
    y, z, core = me // 8, lax.rem(me, 8) // 2, lax.rem(me, 2)
    inner = (z == 1) | (z == 2)
    return core * 4 + jnp.where(inner, 0, 2), y * 2 + z // 2, inner


def kernel(q_hbm, k_hbm, v_hbm, o_ref, q_s, k_s, v_s, w0_s, w1_s, part_s, stat_s, got_p, got_s, near_p, near_s, q_sem, k_sem, v_sem, send_p, send_t, send_o, send_n, send_m, send_x, recv_p, recv_t, recv_o, recv_n, recv_m, recv_x):
    me = lax.axis_index("sp")
    first, quarter, inner = place_of(me)
    w_s = (w0_s, w1_s)

    def give(g):
        r = g % 2
        if g == G - 1:
            for to in (1, 0):
                @pl.when(me != to)
                def _():
                    pltpu.make_async_remote_copy(
                        src_ref=part_s.at[g, pl.ds(2 - 2 * to, 2)], dst_ref=near_p.at[me], send_sem=send_n, recv_sem=recv_n,
                        device_id={"sp": to}, device_id_type=MESH).start()
                    pltpu.make_async_remote_copy(
                        src_ref=stat_s.at[g], dst_ref=near_s.at[me], send_sem=send_m, recv_sem=recv_m,
                        device_id={"sp": to}, device_id_type=MESH).start()

        for c in range(4):
            to = owner_of(g, c)
            if g == G - 1 and to == 1:
                continue

            @pl.when(me != to)
            def _():
                pltpu.make_async_remote_copy(
                    src_ref=part_s.at[g, c], dst_ref=got_p.at[r * N + me], send_sem=send_p, recv_sem=recv_p.at[r],
                    device_id={"sp": to}, device_id_type=MESH).start()
                pltpu.make_async_remote_copy(
                    src_ref=stat_s.at[g], dst_ref=got_s.at[r * N + me], send_sem=send_t, recv_sem=recv_t.at[r],
                    device_id={"sp": to}, device_id_type=MESH).start()

    def whole(ref, send, recv):
        return pltpu.make_async_remote_copy(src_ref=ref, dst_ref=ref, send_sem=send, recv_sem=recv, device_id={"sp": me}, device_id_type=MESH)

    def send(g, c, to, send_sem, recv_sem):
        pltpu.make_async_remote_copy(
            src_ref=o_ref.at[g, c], dst_ref=o_ref.at[g, c], send_sem=send_sem, recv_sem=recv_sem,
            device_id={"sp": to}, device_id_type=MESH).start()

    def together(r):
        g = first + r
        whole(got_s.at[pl.ds(r * N, N - 1)], send_t, recv_t.at[r]).wait_recv()
        whole(got_p.at[pl.ds(r * N, N - 1)], send_p, recv_p.at[r]).wait_recv()
        got_p[r * N + me] = part_s[g, quarter]
        got_s[r * N + me] = stat_s[g]
        highs = [got_s[r * N + j, 0:1] for j in range(N)]
        high = highs[0]
        for h in highs[1:]:
            high = jnp.maximum(high, h)
        seen = jnp.zeros((16, 128), F32)
        total = jnp.zeros((1, 128), F32)
        for j in range(N):
            scale = jnp.exp(highs[j] - high)
            seen = seen + got_p[r * N + j].astype(F32) * scale
            total = total + got_s[r * N + j, 1:2] * scale
        o_ref[g, quarter] = (seen / total).astype(BF16)
        for d in range(N - 1):
            to = d + jnp.where(d >= me, 1, 0)
            if r == 1 and d < 2:
                @pl.when((to >= 2) | (g < G - 1))
                def _():
                    send(g, quarter, to, send_o, recv_o)
            else:
                send(g, quarter, to, send_o, recv_o)

    def together_near():
        g = G - 1
        base = 2 - 2 * me
        whole(near_s.at[pl.ds(0, N - 1)], send_m, recv_m).wait_recv()
        whole(near_p.at[pl.ds(0, N - 1)], send_n, recv_n).wait_recv()
        near_p[me] = part_s[g, pl.ds(base, 2)]
        near_s[me] = stat_s[g]
        highs = [near_s[j, 0:1] for j in range(N)]
        high = highs[0]
        for h in highs[1:]:
            high = jnp.maximum(high, h)
        seen = [jnp.zeros((16, 128), F32)] * 2
        total = jnp.zeros((1, 128), F32)
        for j in range(N):
            scale = jnp.exp(highs[j] - high)
            seen = [seen[c] + near_p[j, c].astype(F32) * scale for c in range(2)]
            total = total + near_s[j, 1:2] * scale
        for c in range(2):
            o_ref[g, base + c] = (seen[c] / total).astype(BF16)
        pltpu.make_async_remote_copy(
            src_ref=o_ref.at[g, pl.ds(base, 2)], dst_ref=o_ref.at[g, pl.ds(base, 2)], send_sem=send_x, recv_sem=recv_x,
            device_id={"sp": 1 - me}, device_id_type=MESH).start()

        @pl.when(me == 1)
        def _():
            for to in range(2, N):
                send(g, 0, to, send_o, recv_o)

    def attend(q_sem, k_sem, v_sem):
        def kcopy(g):
            return pltpu.make_async_copy(k_hbm.at[pl.ds(g * S, S)], k_s.at[pl.ds(g * S, S)], k_sem.at[g])

        def vcopy(g):
            return pltpu.make_async_copy(v_hbm.at[pl.ds(g * S, S)], v_s.at[pl.ds(g * S, S)], v_sem.at[g])

        pltpu.make_async_copy(q_hbm, q_s, q_sem).start()
        kcopy(0).start(priority=1)

        def issue_k(j, _):
            kcopy(j).start(priority=1)
            return 0

        def issue(g, _):
            vcopy(g).start(priority=1)

            @pl.when(g + A + 1 < G)
            def _():
                kcopy(g + A + 1).start(priority=1)

            return 0

        lax.fori_loop(1, A + 1, issue_k, 0)
        lax.fori_loop(0, G, issue, 0)

        barrier = pltpu.get_barrier_semaphore()
        for d in range(1, N):
            pl.semaphore_signal(barrier, inc=1, device_id={"sp": lax.rem(me + d, N)}, device_id_type=MESH)

        lane64 = lax.broadcasted_iota(jnp.int32, (16, 128), 1) // 64
        row4 = lax.broadcasted_iota(jnp.int32, (16, 128), 0) // 4
        lane = lax.broadcasted_iota(jnp.int32, (64, 128), 1) // 4
        rowid = lax.broadcasted_iota(jnp.int32, (16, 128), 0)
        laneid = lax.broadcasted_iota(jnp.int32, (16, 128), 1)

        def scores(g):
            slot = g % 2
            mrow = jnp.zeros((16, 128), F32)
            lrow = jnp.zeros((16, 128), F32)
            for i in range(S):
                qb = q_s[g * S + i].astype(F32)
                qq = jnp.concatenate([qb, qb], -1)
                for t in range(2):
                    piece = qq[16 * t:16 * t + 16]
                    lo = jnp.where(row4 == lane64, piece, 0.0)
                    hi = jnp.where(row4 == lane64 + 2, piece, 0.0)
                    lhs = jnp.concatenate([lo, hi], -1).astype(BF16)
                    s = jnp.dot(lhs, k_s[g * S + i, 256 * t:256 * t + 256, :], preferred_element_type=F32)
                    m = jnp.max(s, -1, keepdims=True)
                    p = jnp.exp((s - m) * 0.125)
                    l = jnp.sum(p, -1, keepdims=True)
                    r = 32 * i + 16 * t
                    w_s[slot][r:r + 16, :] = p.astype(BF16)
                    hit = laneid == rowid + r
                    mrow = jnp.where(hit, m * 0.125, mrow)
                    lrow = jnp.where(hit, l, lrow)
            stat_s[g, 0:1] = jnp.sum(mrow, 0, keepdims=True)
            stat_s[g, 1:2] = jnp.sum(lrow, 0, keepdims=True)

        def values(g):
            w = w_s[g % 2][...]
            acc = jnp.zeros((64, 128), F32)
            for i in range(S):
                res = lax.dot_general(v_s[g * S + i], w, (((1,), (1,)), ((), ())), preferred_element_type=F32)
                for h in range(8):
                    acc = jnp.where(lane == i * 8 + h, res[64 * h:64 * h + 64], acc)
            return acc

        def finish(g, acc):
            part_s[g] = acc.astype(BF16).reshape(4, 16, 128)

        pltpu.make_async_copy(q_hbm, q_s, q_sem).wait()
        kcopy(0).wait()
        scores(0)
        for g in range(G):
            if g + 1 < G:
                kcopy(g + 1).wait()
            vcopy(g).wait()
            if g + 1 < G:
                scores(g + 1)
            finish(g, values(g))
            if g == 0:
                @pl.when(me >= 2)
                def _():
                    pl.semaphore_wait(barrier, N - 1)

            if g == 2:
                @pl.when(me < 2)
                def _():
                    pl.semaphore_wait(barrier, N - 1)
                    give(0)
                    give(1)

            if g < 2:
                @pl.when(me >= 2)
                def _():
                    give(g)
            else:
                give(g)
            if g in (4, 5):
                @pl.when(inner & (first == 0))
                def _():
                    together(g - 4)

    attend(q_sem, k_sem, v_sem)

    @pl.when(jnp.logical_not(inner & (first == 0)))
    def _():
        together(0)

        @pl.when(me != 1)
        def _():
            together(1)

    @pl.when(me < 2)
    def _():
        together_near()

    def tiles(n, send, recv):
        return whole(got_p.at[pl.ds(0, n)], send, recv)

    def stats(n, send, recv):
        return whole(got_s.at[pl.ds(0, n)], send, recv)

    late = (first == G - 2) & (me >= 2)

    @pl.when(me < 2)
    def _():
        tiles(2, send_n, recv_n).wait_send()
        stats(1, send_m, recv_m).wait_send()
        tiles(2, send_x, recv_x).wait()

    @pl.when(me >= 2)
    def _():
        tiles(4, send_n, recv_n).wait_send()
        stats(2, send_m, recv_m).wait_send()
        tiles(30, send_o, recv_o).wait_recv()

    @pl.when(me == 1)
    def _():
        tiles(30, send_p, recv_o).wait_send()
        stats(30, send_t, recv_o).wait_send()
        tiles(29, send_o, recv_o).wait_send()
        tiles(27, send_o, recv_o).wait_recv()

    @pl.when(me == 0)
    def _():
        tiles(26, send_o, recv_o).wait_recv()

    @pl.when(late)
    def _():
        tiles(29, send_p, recv_o).wait_send()
        stats(29, send_t, recv_o).wait_send()
        tiles(28, send_o, recv_o).wait_send()

    @pl.when(jnp.logical_not(late) & (me != 1))
    def _():
        tiles(29, send_p, recv_o).wait_send()
        stats(29, send_t, recv_o).wait_send()
        tiles(30, send_o, recv_o).wait_send()


def solution(mesh):
    def step(q, k, v):
        k = jnp.transpose(k, (0, 2, 3, 1)).reshape(32, 512, 512)
        v = jnp.transpose(v, (0, 2, 3, 1)).reshape(32, 512, 512)
        o = pl.pallas_call(
            kernel,
            out_shape=pltpu.VMEM((G, 4, 16, 128), BF16),
            in_specs=[pl.BlockSpec(memory_space=pl.ANY)] * 3,
            out_specs=pl.BlockSpec(memory_space=pltpu.VMEM),
            scratch_shapes=[
                pltpu.VMEM((32, 32, 64), BF16),
                pltpu.VMEM((32, 512, 512), BF16),
                pltpu.VMEM((32, 512, 512), BF16),
                pltpu.VMEM((128, 512), BF16),
                pltpu.VMEM((128, 512), BF16),
                pltpu.VMEM((G, 4, 16, 128), BF16),
                pltpu.VMEM((G, 2, 128), F32),
                pltpu.VMEM((2 * N, 16, 128), BF16),
                pltpu.VMEM((2 * N, 2, 128), F32),
                pltpu.VMEM((N, 2, 16, 128), BF16),
                pltpu.VMEM((N, 2, 128), F32),
                pltpu.SemaphoreType.DMA(()),
                pltpu.SemaphoreType.DMA((G,)),
                pltpu.SemaphoreType.DMA((G,)),
                pltpu.SemaphoreType.DMA(()),
                pltpu.SemaphoreType.DMA(()),
                pltpu.SemaphoreType.DMA(()),
                pltpu.SemaphoreType.DMA(()),
                pltpu.SemaphoreType.DMA(()),
                pltpu.SemaphoreType.DMA(()),
                pltpu.SemaphoreType.DMA((2,)),
                pltpu.SemaphoreType.DMA((2,)),
                pltpu.SemaphoreType.DMA(()),
                pltpu.SemaphoreType.DMA(()),
                pltpu.SemaphoreType.DMA(()),
                pltpu.SemaphoreType.DMA(()),
            ],
            compiler_params=pltpu.CompilerParams(vmem_limit_bytes=56 << 20, collective_id=0, has_side_effects=True),
        )(q, k, v)
        return o.reshape(G, 64, 128).transpose(0, 2, 1).reshape(32, 32, 64)

    return jax.shard_map(
        step,
        mesh=mesh,
        in_specs=(P("dp", None, None), P("dp", "sp", None, None), P("dp", "sp", None, None)),
        out_specs=P("dp", None, None),
        check_vma=False,
    )
```

```python
import jax
import jax.numpy as jnp
from jax import lax
from jax.experimental import pallas as pl
from jax.experimental.pallas import tpu as pltpu
from jax.sharding import PartitionSpec as P

MESH = pl.DeviceIdType.MESH
F32, BF16 = jnp.float32, jnp.bfloat16
N = 16
G = 8
S = 4
A = 1


def owners_of(g):
    if g in (2, 3):
        return [(0, 0, 2), (8, 2, 2)]
    outer = g // 4 * (g // 2 % 2)
    zs = (0, 3) if outer else (1, 2)
    who = [((c // 2 * 4 + zs[c % 2]) * 2 + g // 4, c, 1) for c in range(4)]
    return who[1:] if g == G - 1 else who


def near_half(to):
    return 2 - 2 * to


def kernel(q_hbm, k_hbm, v_hbm, o_ref, q_s, k_s, v_s, w0_s, w1_s, part_s, stat_s, got_p, got_s, pair_p, near_p, near_s, send_p, send_t, send_o, send_n, send_m, send_x, recv_p, recv_t, recv_o, recv_n, recv_m, recv_x):
    me = lax.axis_index("sp")
    y, z, core = me // 8, lax.rem(me, 8) // 2, lax.rem(me, 2)
    inner, edge, far = (z == 1) | (z == 2), z == 0, z == 3
    first = core * 4 + jnp.where(inner, 0, 2)
    quarter, base = y * 2 + z // 2, y * 2
    w_s = (w0_s, w1_s)

    def pass_on(g, c, n, to, dst_p, dst_s, sems):
        @pl.when(me != to)
        def _():
            src = part_s.at[g, c] if n == 1 else part_s.at[g, pl.ds(c, n)]
            pltpu.make_async_remote_copy(
                src_ref=src, dst_ref=dst_p, send_sem=sems[0], recv_sem=sems[1], device_id={"sp": to}, device_id_type=MESH).start()
            pltpu.make_async_remote_copy(
                src_ref=stat_s.at[g], dst_ref=dst_s, send_sem=sems[2], recv_sem=sems[3], device_id={"sp": to}, device_id_type=MESH).start()

    def give(g):
        r = g % 2
        if g == G - 1:
            for to in (1, 0):
                pass_on(g, near_half(to), 2, to, near_p.at[me], near_s.at[me], (send_n, recv_n, send_m, recv_m))
        for to, c, n in owners_of(g):
            dst = got_p.at[r * N + me] if n == 1 else pair_p.at[r * N + me]
            pass_on(g, c, n, to, dst, got_s.at[r * N + me], (send_p, recv_p.at[r], send_t, recv_t.at[r]))

    def whole(ref, send, recv):
        return pltpu.make_async_remote_copy(src_ref=ref, dst_ref=ref, send_sem=send, recv_sem=recv, device_id={"sp": me}, device_id_type=MESH)

    def send(ref, to, send_sem, recv_sem):
        pltpu.make_async_remote_copy(
            src_ref=ref, dst_ref=ref, send_sem=send_sem, recv_sem=recv_sem, device_id={"sp": to}, device_id_type=MESH).start()

    def scales(stat, at):
        highs = [stat[at + j, 0:1] for j in range(N)]
        high = highs[0]
        for h in highs[1:]:
            high = jnp.maximum(high, h)
        scale = [jnp.exp(h - high) for h in highs]
        total = jnp.zeros((1, 128), F32)
        for j in range(N):
            total = total + stat[at + j, 1:2] * scale[j]
        return scale, total

    def together_one(r):
        g = first + r
        whole(got_s.at[pl.ds(r * N, N - 1)], send_t, recv_t.at[r]).wait_recv()
        whole(got_p.at[pl.ds(r * N, N - 1)], send_p, recv_p.at[r]).wait_recv()
        got_p[r * N + me] = part_s[g, quarter]
        got_s[r * N + me] = stat_s[g]
        scale, total = scales(got_s, r * N)
        seen = jnp.zeros((16, 128), F32)
        for j in range(N):
            seen = seen + got_p[r * N + j].astype(F32) * scale[j]
        o_ref[g, quarter] = (seen / total).astype(BF16)
        for d in range(N - 1):
            to = d + jnp.where(d >= me, 1, 0)
            if r == 1 and d < 2:
                @pl.when((g < G - 1) | (to >= 2))
                def _():
                    send(o_ref.at[g, quarter], to, send_o, recv_o)
            else:
                send(o_ref.at[g, quarter], to, send_o, recv_o)

    def join(src_p, src_s, at, g, c):
        src_p[at + me] = part_s[g, pl.ds(c, 2)]
        src_s[at + me] = stat_s[g]
        scale, total = scales(src_s, at)
        seen = [jnp.zeros((16, 128), F32)] * 2
        for j in range(N):
            seen = [seen[i] + src_p[at + j, i].astype(F32) * scale[j] for i in range(2)]
        for i in range(2):
            o_ref[g, c + i] = (seen[i] / total).astype(BF16)

    def together_two(r):
        g = first + r
        whole(got_s.at[pl.ds(r * N, N - 1)], send_t, recv_t.at[r]).wait_recv()
        whole(pair_p.at[pl.ds(r * N, N - 1)], send_p, recv_p.at[r]).wait_recv()
        join(pair_p, got_s, r * N, g, base)
        for d in range(N - 1):
            send(o_ref.at[g, pl.ds(base, 2)], d + jnp.where(d >= me, 1, 0), send_o, recv_o)

    def together_near():
        whole(near_s.at[pl.ds(0, N - 1)], send_m, recv_m).wait_recv()
        whole(near_p.at[pl.ds(0, N - 1)], send_n, recv_n).wait_recv()
        half = near_half(me)
        join(near_p, near_s, 0, G - 1, half)
        send(o_ref.at[G - 1, pl.ds(half, 2)], 1 - me, send_x, recv_x)

        @pl.when(me == 1)
        def _():
            for to in range(2, N):
                send(o_ref.at[G - 1, 0], to, send_o, recv_o)

    def attend(q_sem, k_sem, v_sem):
        def kcopy(g):
            return pltpu.make_async_copy(k_hbm.at[pl.ds(g * S, S)], k_s.at[pl.ds(g * S, S)], k_sem.at[g])

        def vcopy(g):
            return pltpu.make_async_copy(v_hbm.at[pl.ds(g * S, S)], v_s.at[pl.ds(g * S, S)], v_sem.at[g])

        pltpu.make_async_copy(q_hbm, q_s, q_sem).start()
        kcopy(0).start(priority=1)

        def issue_k(j, _):
            kcopy(j).start(priority=1)
            return 0

        def issue(g, _):
            vcopy(g).start(priority=1)

            @pl.when(g + A + 1 < G)
            def _():
                kcopy(g + A + 1).start(priority=1)

            return 0

        lax.fori_loop(1, A + 1, issue_k, 0)
        lax.fori_loop(0, G, issue, 0)

        barrier = pltpu.get_barrier_semaphore()
        for d in range(1, N):
            pl.semaphore_signal(barrier, inc=1, device_id={"sp": lax.rem(me + d, N)}, device_id_type=MESH)

        lane64 = lax.broadcasted_iota(jnp.int32, (16, 128), 1) // 64
        row4 = lax.broadcasted_iota(jnp.int32, (16, 128), 0) // 4
        lane = lax.broadcasted_iota(jnp.int32, (64, 128), 1) // 4
        rowid = lax.broadcasted_iota(jnp.int32, (16, 128), 0)
        laneid = lax.broadcasted_iota(jnp.int32, (16, 128), 1)

        def scores(g):
            slot = g % 2
            mrow = jnp.zeros((16, 128), F32)
            lrow = jnp.zeros((16, 128), F32)
            for i in range(S):
                qb = q_s[g * S + i].astype(F32)
                qq = jnp.concatenate([qb, qb], -1)
                for t in range(2):
                    piece = qq[16 * t:16 * t + 16]
                    lo = jnp.where(row4 == lane64, piece, 0.0)
                    hi = jnp.where(row4 == lane64 + 2, piece, 0.0)
                    lhs = jnp.concatenate([lo, hi], -1).astype(BF16)
                    s = jnp.dot(lhs, k_s[g * S + i, 256 * t:256 * t + 256, :], preferred_element_type=F32)
                    m = jnp.max(s, -1, keepdims=True)
                    p = jnp.exp((s - m) * 0.125)
                    l = jnp.sum(p, -1, keepdims=True)
                    r = 32 * i + 16 * t
                    w_s[slot][r:r + 16, :] = p.astype(BF16)
                    hit = laneid == rowid + r
                    mrow = jnp.where(hit, m * 0.125, mrow)
                    lrow = jnp.where(hit, l, lrow)
            stat_s[g, 0:1] = jnp.sum(mrow, 0, keepdims=True)
            stat_s[g, 1:2] = jnp.sum(lrow, 0, keepdims=True)

        def values(g):
            w = w_s[g % 2][...]
            acc = jnp.zeros((64, 128), F32)
            for i in range(S):
                res = lax.dot_general(v_s[g * S + i], w, (((1,), (1,)), ((), ())), preferred_element_type=F32)
                for h in range(8):
                    acc = jnp.where(lane == i * 8 + h, res[64 * h:64 * h + 64], acc)
            return acc

        def finish(g, acc):
            part_s[g] = acc.astype(BF16).reshape(4, 16, 128)

        pltpu.make_async_copy(q_hbm, q_s, q_sem).wait()
        kcopy(0).wait()
        scores(0)
        for g in range(G):
            if g + 1 < G:
                kcopy(g + 1).wait()
            vcopy(g).wait()
            if g + 1 < G:
                scores(g + 1)
            finish(g, values(g))
            if g == 0:
                @pl.when(me >= 2)
                def _():
                    pl.semaphore_wait(barrier, N - 1)

            if g == 2:
                @pl.when(me < 2)
                def _():
                    pl.semaphore_wait(barrier, N - 1)
                    give(0)
                    give(1)

            if g < 2:
                @pl.when(me >= 2)
                def _():
                    give(g)
            else:
                give(g)
            if g in (4, 5):
                @pl.when(inner & (core == 0))
                def _():
                    together_one(g - 4)

    pl.run_scoped(attend, pltpu.SemaphoreType.DMA(()), pltpu.SemaphoreType.DMA((G,)), pltpu.SemaphoreType.DMA((G,)))

    @pl.when(core == 1)
    def _():
        together_one(0)

        @pl.when(me != 1)
        def _():
            together_one(1)

    @pl.when(edge & (core == 0))
    def _():
        together_two(0)
        together_two(1)

    @pl.when(me < 2)
    def _():
        together_near()

    def tiles(n, send, recv):
        return whole(got_p.at[pl.ds(0, n)] if n <= 2 * N else pair_p.at[pl.ds(0, n // 2)], send, recv)

    def stats(n, send, recv):
        return whole(got_s.at[pl.ds(0, n)], send, recv)

    for which, halves in ((me < 2, 1), (me >= 2, 2)):
        @pl.when(which)
        def _():
            tiles(2 * halves, send_n, recv_n).wait_send()
            stats(halves, send_m, recv_m).wait_send()

    pair, idle, outer = edge & (core == 0), far & (core == 0), (core == 1) & (edge | far) & (me != 1)
    for which, parts, shares, results in ((idle, 31, 27, 0), (inner, 29, 25, 30), (outer, 29, 25, 28), (pair, 27, 25, 60), (me == 1, 30, 26, 29)):
        @pl.when(which)
        def _():
            tiles(parts, send_p, recv_o).wait_send()
            stats(shares, send_t, recv_o).wait_send()
            if results:
                tiles(results, send_o, recv_o).wait_send()

    for which, results in ((idle, 32), (inner | outer, 30), (me == 8, 28), (me == 1, 27), (me == 0, 24)):
        @pl.when(which)
        def _():
            tiles(results, send_o, recv_o).wait_recv()

    @pl.when(me < 2)
    def _():
        tiles(2, send_x, recv_x).wait()


def solution(mesh):
    def step(q, k, v):
        k = jnp.transpose(k, (0, 2, 3, 1)).reshape(32, 512, 512)
        v = jnp.transpose(v, (0, 2, 3, 1)).reshape(32, 512, 512)
        o = pl.pallas_call(
            kernel,
            out_shape=pltpu.VMEM((G, 4, 16, 128), BF16),
            in_specs=[pl.BlockSpec(memory_space=pl.ANY)] * 3,
            out_specs=pl.BlockSpec(memory_space=pltpu.VMEM),
            scratch_shapes=[
                pltpu.VMEM((32, 32, 64), BF16),
                pltpu.VMEM((32, 512, 512), BF16),
                pltpu.VMEM((32, 512, 512), BF16),
                pltpu.VMEM((128, 512), BF16),
                pltpu.VMEM((128, 512), BF16),
                pltpu.VMEM((G, 4, 16, 128), BF16),
                pltpu.VMEM((G, 2, 128), F32),
                pltpu.VMEM((2 * N, 16, 128), BF16),
                pltpu.VMEM((2 * N, 2, 128), F32),
                pltpu.VMEM((2 * N, 2, 16, 128), BF16),
                pltpu.VMEM((N, 2, 16, 128), BF16),
                pltpu.VMEM((N, 2, 128), F32),
                pltpu.SemaphoreType.DMA(()),
                pltpu.SemaphoreType.DMA(()),
                pltpu.SemaphoreType.DMA(()),
                pltpu.SemaphoreType.DMA(()),
                pltpu.SemaphoreType.DMA(()),
                pltpu.SemaphoreType.DMA(()),
                pltpu.SemaphoreType.DMA((2,)),
                pltpu.SemaphoreType.DMA((2,)),
                pltpu.SemaphoreType.DMA(()),
                pltpu.SemaphoreType.DMA(()),
                pltpu.SemaphoreType.DMA(()),
                pltpu.SemaphoreType.DMA(()),
            ],
            compiler_params=pltpu.CompilerParams(vmem_limit_bytes=56 << 20, collective_id=0, has_side_effects=True),
        )(q, k, v)
        return o.reshape(G, 64, 128).transpose(0, 2, 1).reshape(32, 32, 64)

    return jax.shard_map(
        step,
        mesh=mesh,
        in_specs=(P("dp", None, None), P("dp", "sp", None, None), P("dp", "sp", None, None)),
        out_specs=P("dp", None, None),
        check_vma=False,
    )
```

```python
import jax
import jax.numpy as jnp
from jax import lax
from jax.experimental import pallas as pl
from jax.experimental.pallas import tpu as pltpu
from jax.sharding import PartitionSpec as P

MESH = pl.DeviceIdType.MESH
F32, BF16 = jnp.float32, jnp.bfloat16
N = 16
G = 8
S = 4
A = 1


def owners_of(g):
    if g in (2, 3):
        return [(0, 0, 2), (8, 2, 2)]
    outer = g // 4 * (g // 2 % 2)
    zs = (0, 3) if outer else (1, 2)
    who = [((c // 2 * 4 + zs[c % 2]) * 2 + g // 4, c, 1) for c in range(4)]
    return who[1:] if g == G - 1 else who


def kernel(q_hbm, k_hbm, v_hbm, o_ref, q_s, k_s, v_s, w0_s, w1_s, part_s, stat_s, got_p, got_s, pair_p, near_p, near_s, gauge, sent, recv, recv_o, recv_n, recv_x):
    me = lax.axis_index("sp")
    y, z, core = me // 8, lax.rem(me, 8) // 2, lax.rem(me, 2)
    inner, edge, far = (z == 1) | (z == 2), z == 0, z == 3
    first = core * 4 + jnp.where(inner, 0, 2)
    quarter, base = y * 2 + z // 2, y * 2
    w_s = (w0_s, w1_s)

    def copy(src, dst, to, sem):
        pltpu.make_async_remote_copy(src_ref=src, dst_ref=dst, send_sem=sent, recv_sem=sem, device_id={"sp": to}, device_id_type=MESH).start()

    def give(g):
        r = g % 2
        if g == G - 1:
            @pl.when(me != 1)
            def _():
                copy(part_s.at[g], near_p.at[me], 1, recv_n)
                copy(stat_s.at[g], near_s.at[me], 1, recv_n)

        for to, c, n in owners_of(g):
            @pl.when(me != to)
            def _():
                if n == 1:
                    copy(part_s.at[g, c], got_p.at[r * N + me], to, recv.at[r])
                else:
                    copy(part_s.at[g, pl.ds(c, n)], pair_p.at[r * N + me], to, recv.at[r])
                copy(stat_s.at[g], got_s.at[r * N + me], to, recv.at[r])

    def wait_recv(kib, sem):
        pltpu.make_async_remote_copy(
            src_ref=gauge.at[pl.ds(0, kib)], dst_ref=gauge.at[pl.ds(0, kib)], send_sem=sent, recv_sem=sem,
            device_id={"sp": me}, device_id_type=MESH).wait_recv()

    def wait_sent(kib):
        pltpu.make_async_remote_copy(
            src_ref=gauge.at[pl.ds(0, kib)], dst_ref=gauge.at[pl.ds(0, kib)], send_sem=sent, recv_sem=recv_o,
            device_id={"sp": me}, device_id_type=MESH).wait_send()

    def add_up(tiles, stat, at, n, c):
        highs = [stat[at + j, 0:1] for j in range(n)]
        high = highs[0]
        for h in highs[1:]:
            high = jnp.maximum(high, h)
        seen = [jnp.zeros((16, 128), F32)] * c
        total = jnp.zeros((1, 128), F32)
        for j in range(n):
            scale = jnp.exp(highs[j] - high)
            seen = [seen[i] + tiles(at + j, i).astype(F32) * scale for i in range(c)]
            total = total + stat[at + j, 1:2] * scale
        return seen, total, high

    def together_one(r):
        g = first + r
        wait_recv(5 * (N - 1), recv.at[r])
        got_p[r * N + me] = part_s[g, quarter]
        got_s[r * N + me] = stat_s[g]
        seen, total, _ = add_up(lambda j, i: got_p[j], got_s, r * N, N, 1)
        o_ref[g, quarter] = (seen[0] / total).astype(BF16)
        for d in range(N - 1):
            to = d + jnp.where(d >= me, 1, 0)
            if r == 1 and d < 2:
                @pl.when((g < G - 1) | (to >= 2))
                def _():
                    copy(o_ref.at[g, quarter], o_ref.at[g, quarter], to, recv_o)
            else:
                copy(o_ref.at[g, quarter], o_ref.at[g, quarter], to, recv_o)

    def together_two(r):
        g = first + r
        wait_recv(9 * (N - 1), recv.at[r])
        pair_p[r * N + me] = part_s[g, pl.ds(base, 2)]
        got_s[r * N + me] = stat_s[g]
        seen, total, _ = add_up(lambda j, i: pair_p[j, i], got_s, r * N, N, 2)
        for i in range(2):
            o_ref[g, base + i] = (seen[i] / total).astype(BF16)
        for d in range(N - 1):
            half = o_ref.at[g, pl.ds(base, 2)]
            copy(half, half, d + jnp.where(d >= me, 1, 0), recv_o)

    def together_near():
        g = G - 1
        wait_recv(17 * (N - 1), recv_n)
        near_p[me] = part_s[g]
        near_s[me] = stat_s[g]
        seen, total, _ = add_up(lambda j, i: near_p[j, i], near_s, 0, N, 4)
        for i in range(4):
            o_ref[g, i] = (seen[i] / total).astype(BF16)
        copy(o_ref.at[g], o_ref.at[g], 0, recv_x)
        for to in range(2, N):
            copy(o_ref.at[g, 0], o_ref.at[g, 0], to, recv_o)

    def attend(q_sem, k_sem, v_sem):
        def kcopy(g):
            return pltpu.make_async_copy(k_hbm.at[pl.ds(g * S, S)], k_s.at[pl.ds(g * S, S)], k_sem.at[g])

        def vcopy(g):
            return pltpu.make_async_copy(v_hbm.at[pl.ds(g * S, S)], v_s.at[pl.ds(g * S, S)], v_sem.at[g])

        pltpu.make_async_copy(q_hbm, q_s, q_sem).start()
        kcopy(0).start(priority=1)

        def issue_k(j, _):
            kcopy(j).start(priority=1)
            return 0

        def issue(g, _):
            vcopy(g).start(priority=1)

            @pl.when(g + A + 1 < G)
            def _():
                kcopy(g + A + 1).start(priority=1)

            return 0

        lax.fori_loop(1, A + 1, issue_k, 0)
        lax.fori_loop(0, G, issue, 0)

        barrier = pltpu.get_barrier_semaphore()
        for d in range(1, N):
            pl.semaphore_signal(barrier, inc=1, device_id={"sp": lax.rem(me + d, N)}, device_id_type=MESH)

        lane64 = lax.broadcasted_iota(jnp.int32, (16, 128), 1) // 64
        row4 = lax.broadcasted_iota(jnp.int32, (16, 128), 0) // 4
        lane = lax.broadcasted_iota(jnp.int32, (64, 128), 1) // 4
        rowid = lax.broadcasted_iota(jnp.int32, (16, 128), 0)
        laneid = lax.broadcasted_iota(jnp.int32, (16, 128), 1)

        def scores(g):
            slot = g % 2
            mrow = jnp.zeros((16, 128), F32)
            lrow = jnp.zeros((16, 128), F32)
            for i in range(S):
                qb = q_s[g * S + i].astype(F32)
                qq = jnp.concatenate([qb, qb], -1)
                for t in range(2):
                    piece = qq[16 * t:16 * t + 16]
                    lo = jnp.where(row4 == lane64, piece, 0.0)
                    hi = jnp.where(row4 == lane64 + 2, piece, 0.0)
                    lhs = jnp.concatenate([lo, hi], -1).astype(BF16)
                    s = jnp.dot(lhs, k_s[g * S + i, 256 * t:256 * t + 256, :], preferred_element_type=F32)
                    m = jnp.max(s, -1, keepdims=True)
                    p = jnp.exp((s - m) * 0.125)
                    l = jnp.sum(p, -1, keepdims=True)
                    r = 32 * i + 16 * t
                    w_s[slot][r:r + 16, :] = p.astype(BF16)
                    hit = laneid == rowid + r
                    mrow = jnp.where(hit, m * 0.125, mrow)
                    lrow = jnp.where(hit, l, lrow)
            stat_s[g, 0:1] = jnp.sum(mrow, 0, keepdims=True)
            stat_s[g, 1:2] = jnp.sum(lrow, 0, keepdims=True)

        def values(g):
            w = w_s[g % 2][...]
            acc = jnp.zeros((64, 128), F32)
            for i in range(S):
                res = lax.dot_general(v_s[g * S + i], w, (((1,), (1,)), ((), ())), preferred_element_type=F32)
                for h in range(8):
                    acc = jnp.where(lane == i * 8 + h, res[64 * h:64 * h + 64], acc)
            return acc

        def finish(g, acc):
            part_s[g] = acc.astype(BF16).reshape(4, 16, 128)

        pltpu.make_async_copy(q_hbm, q_s, q_sem).wait()
        kcopy(0).wait()
        scores(0)
        for g in range(G):
            if g + 1 < G:
                kcopy(g + 1).wait()
            vcopy(g).wait()
            if g + 1 < G:
                scores(g + 1)
            finish(g, values(g))
            if g == 0:
                @pl.when(me >= 2)
                def _():
                    pl.semaphore_wait(barrier, N - 1)

            if g == 2:
                @pl.when(me < 2)
                def _():
                    pl.semaphore_wait(barrier, N - 1)
                    give(0)
                    give(1)

            if g < 2:
                @pl.when(me >= 2)
                def _():
                    give(g)
            else:
                give(g)
            if g in (4, 5):
                @pl.when(inner & (core == 0))
                def _():
                    together_one(g - 4)

    pl.run_scoped(attend, pltpu.SemaphoreType.DMA(()), pltpu.SemaphoreType.DMA((G,)), pltpu.SemaphoreType.DMA((G,)))

    @pl.when(core == 1)
    def _():
        together_one(0)

        @pl.when(me != 1)
        def _():
            together_one(1)

    @pl.when(edge & (core == 0))
    def _():
        together_two(0)
        together_two(1)

    @pl.when(me == 1)
    def _():
        together_near()

    pair, idle, last = edge & (core == 0), far & (core == 0), (core == 1) & (edge | far) & (me != 1)

    for which, kib in ((idle, 168), (inner, 278), (last, 270), (pair, 390), (me == 1, 278)):
        @pl.when(which)
        def _():
            wait_sent(kib)

    for which, kib in ((idle, 128), (inner | last, 120), (me == 8, 112), (me == 1, 108), (me == 0, 96)):
        @pl.when(which)
        def _():
            wait_recv(kib, recv_o)

    @pl.when(me == 0)
    def _():
        wait_recv(16, recv_x)


def solution(mesh):
    def step(q, k, v):
        k = jnp.transpose(k, (0, 2, 3, 1)).reshape(32, 512, 512)
        v = jnp.transpose(v, (0, 2, 3, 1)).reshape(32, 512, 512)
        o = pl.pallas_call(
            kernel,
            out_shape=pltpu.VMEM((G, 4, 16, 128), BF16),
            in_specs=[pl.BlockSpec(memory_space=pl.ANY)] * 3,
            out_specs=pl.BlockSpec(memory_space=pltpu.VMEM),
            scratch_shapes=[
                pltpu.VMEM((32, 32, 64), BF16),
                pltpu.VMEM((32, 512, 512), BF16),
                pltpu.VMEM((32, 512, 512), BF16),
                pltpu.VMEM((128, 512), BF16),
                pltpu.VMEM((128, 512), BF16),
                pltpu.VMEM((G, 4, 16, 128), BF16),
                pltpu.VMEM((G, 2, 128), F32),
                pltpu.VMEM((2 * N, 16, 128), BF16),
                pltpu.VMEM((2 * N, 2, 128), F32),
                pltpu.VMEM((2 * N, 2, 16, 128), BF16),
                pltpu.VMEM((N, 4, 16, 128), BF16),
                pltpu.VMEM((N, 2, 128), F32),
                pltpu.VMEM((400, 2, 128), F32),
                pltpu.SemaphoreType.DMA(()),
                pltpu.SemaphoreType.DMA((2,)),
                pltpu.SemaphoreType.DMA(()),
                pltpu.SemaphoreType.DMA(()),
                pltpu.SemaphoreType.DMA(()),
            ],
            compiler_params=pltpu.CompilerParams(vmem_limit_bytes=56 << 20, collective_id=0, has_side_effects=True),
        )(q, k, v)
        return o.reshape(G, 64, 128).transpose(0, 2, 1).reshape(32, 32, 64)

    return jax.shard_map(
        step,
        mesh=mesh,
        in_specs=(P("dp", None, None), P("dp", "sp", None, None), P("dp", "sp", None, None)),
        out_specs=P("dp", None, None),
        check_vma=False,
    )
```

```python
import jax
import jax.numpy as jnp
from jax import lax
from jax.experimental import pallas as pl
from jax.experimental.pallas import tpu as pltpu
from jax.sharding import PartitionSpec as P

MESH = pl.DeviceIdType.MESH
F32, BF16 = jnp.float32, jnp.bfloat16
N = 16
G = 8
S = 4
A = 1


def owners_of(g):
    if g in (2, 3):
        return [(0, 0, 2), (8, 2, 2)]
    if g >= 6:
        return [(1, 0, 1), (9, 1, 1), (15, 2, 2)][g - 6:]
    return [((c // 2 * 4 + 1 + c % 2) * 2 + g // 4, c, 1) for c in range(4)]


def kernel(q_hbm, k_hbm, v_hbm, o_ref, q_s, k_s, v_s, w0_s, w1_s, part_s, stat_s, got_p, got_s, pair_p, near_p, near_s, gauge, sent, recv, recv_o, recv_n, recv_x):
    me = lax.axis_index("sp")
    y, z, core = me // 8, lax.rem(me, 8) // 2, lax.rem(me, 2)
    inner, edge, far = (z == 1) | (z == 2), z == 0, z == 3
    first = core * 4 + jnp.where(inner, 0, 2)
    quarter, base = jnp.where(me == 9, 1, y * 2 + z // 2), y * 2
    w_s = (w0_s, w1_s)

    def copy(src, dst, to, sem):
        pltpu.make_async_remote_copy(src_ref=src, dst_ref=dst, send_sem=sent, recv_sem=sem, device_id={"sp": to}, device_id_type=MESH).start()

    def give(g):
        r = g % 2
        if g == G - 1:
            @pl.when(me != 1)
            def _():
                copy(part_s.at[g], near_p.at[me], 1, recv_n)
                copy(stat_s.at[g], near_s.at[me], 1, recv_n)

        for to, c, n in owners_of(g):
            @pl.when(me != to)
            def _():
                if n == 1:
                    copy(part_s.at[g, c], got_p.at[r * N + me], to, recv.at[r])
                else:
                    copy(part_s.at[g, pl.ds(c, n)], pair_p.at[r * N + me], to, recv.at[r])
                copy(stat_s.at[g], got_s.at[r * N + me], to, recv.at[r])

    def wait_recv(kib, sem):
        pltpu.make_async_remote_copy(
            src_ref=gauge.at[pl.ds(0, kib)], dst_ref=gauge.at[pl.ds(0, kib)], send_sem=sent, recv_sem=sem,
            device_id={"sp": me}, device_id_type=MESH).wait_recv()

    def wait_sent(kib):
        pltpu.make_async_remote_copy(
            src_ref=gauge.at[pl.ds(0, kib)], dst_ref=gauge.at[pl.ds(0, kib)], send_sem=sent, recv_sem=recv_o,
            device_id={"sp": me}, device_id_type=MESH).wait_send()

    def add_up(tiles, stat, at, n, c):
        highs = [stat[at + j, 0:1] for j in range(n)]
        high = highs[0]
        for h in highs[1:]:
            high = jnp.maximum(high, h)
        seen = [jnp.zeros((16, 128), F32)] * c
        total = jnp.zeros((1, 128), F32)
        for j in range(n):
            scale = jnp.exp(highs[j] - high)
            seen = [seen[i] + tiles(at + j, i).astype(F32) * scale for i in range(c)]
            total = total + stat[at + j, 1:2] * scale
        return seen, total, high

    def together_one(r):
        g = first + r
        wait_recv(5 * (N - 1), recv.at[r])
        got_p[r * N + me] = part_s[g, quarter]
        got_s[r * N + me] = stat_s[g]
        seen, total, _ = add_up(lambda j, i: got_p[j], got_s, r * N, N, 1)
        o_ref[g, quarter] = (seen[0] / total).astype(BF16)
        for d in range(N - 1):
            to = d + jnp.where(d >= me, 1, 0)
            if r == 1 and d < 2:
                @pl.when((g < G - 1) | (to >= 2))
                def _():
                    copy(o_ref.at[g, quarter], o_ref.at[g, quarter], to, recv_o)
            else:
                copy(o_ref.at[g, quarter], o_ref.at[g, quarter], to, recv_o)

    def together_two(r):
        g = first + r
        wait_recv(9 * (N - 1), recv.at[r])
        pair_p[r * N + me] = part_s[g, pl.ds(base, 2)]
        got_s[r * N + me] = stat_s[g]
        seen, total, _ = add_up(lambda j, i: pair_p[j, i], got_s, r * N, N, 2)
        for i in range(2):
            o_ref[g, base + i] = (seen[i] / total).astype(BF16)
        half = o_ref.at[g, pl.ds(base, 2)]
        for d in range(N - 1):
            to = d + jnp.where(d >= me, 1, 0)
            if r == 1 and d < 2:
                @pl.when((g < G - 1) | (to >= 2))
                def _():
                    copy(half, half, to, recv_o)
            else:
                copy(half, half, to, recv_o)

    def together_near():
        g = G - 1
        wait_recv(17 * (N - 1), recv_n)
        near_p[me] = part_s[g]
        near_s[me] = stat_s[g]
        seen, total, _ = add_up(lambda j, i: near_p[j, i], near_s, 0, N, 4)
        for i in range(4):
            o_ref[g, i] = (seen[i] / total).astype(BF16)
        copy(o_ref.at[g], o_ref.at[g], 0, recv_x)
        for to in range(2, N):
            copy(o_ref.at[g, 0], o_ref.at[g, 0], to, recv_o)

    def attend(q_sem, k_sem, v_sem):
        def kcopy(g):
            return pltpu.make_async_copy(k_hbm.at[pl.ds(g * S, S)], k_s.at[pl.ds(g * S, S)], k_sem.at[g])

        def vcopy(g):
            return pltpu.make_async_copy(v_hbm.at[pl.ds(g * S, S)], v_s.at[pl.ds(g * S, S)], v_sem.at[g])

        pltpu.make_async_copy(q_hbm, q_s, q_sem).start()
        kcopy(0).start(priority=1)

        def issue_k(j, _):
            kcopy(j).start(priority=1)
            return 0

        def issue(g, _):
            vcopy(g).start(priority=1)

            @pl.when(g + A + 1 < G)
            def _():
                kcopy(g + A + 1).start(priority=1)

            return 0

        lax.fori_loop(1, A + 1, issue_k, 0)
        lax.fori_loop(0, G, issue, 0)

        barrier = pltpu.get_barrier_semaphore()
        for d in range(1, N):
            pl.semaphore_signal(barrier, inc=1, device_id={"sp": lax.rem(me + d, N)}, device_id_type=MESH)

        lane64 = lax.broadcasted_iota(jnp.int32, (16, 128), 1) // 64
        row4 = lax.broadcasted_iota(jnp.int32, (16, 128), 0) // 4
        lane = lax.broadcasted_iota(jnp.int32, (64, 128), 1) // 4
        rowid = lax.broadcasted_iota(jnp.int32, (16, 128), 0)
        laneid = lax.broadcasted_iota(jnp.int32, (16, 128), 1)

        def scores(g):
            slot = g % 2
            mrow = jnp.zeros((16, 128), F32)
            lrow = jnp.zeros((16, 128), F32)
            for i in range(S):
                qb = q_s[g * S + i].astype(F32)
                qq = jnp.concatenate([qb, qb], -1)
                for t in range(2):
                    piece = qq[16 * t:16 * t + 16]
                    lo = jnp.where(row4 == lane64, piece, 0.0)
                    hi = jnp.where(row4 == lane64 + 2, piece, 0.0)
                    lhs = jnp.concatenate([lo, hi], -1).astype(BF16)
                    s = jnp.dot(lhs, k_s[g * S + i, 256 * t:256 * t + 256, :], preferred_element_type=F32)
                    m = jnp.max(s, -1, keepdims=True)
                    p = jnp.exp((s - m) * 0.125)
                    l = jnp.sum(p, -1, keepdims=True)
                    r = 32 * i + 16 * t
                    w_s[slot][r:r + 16, :] = p.astype(BF16)
                    hit = laneid == rowid + r
                    mrow = jnp.where(hit, m * 0.125, mrow)
                    lrow = jnp.where(hit, l, lrow)
            stat_s[g, 0:1] = jnp.sum(mrow, 0, keepdims=True)
            stat_s[g, 1:2] = jnp.sum(lrow, 0, keepdims=True)

        def values(g):
            w = w_s[g % 2][...]
            acc = jnp.zeros((64, 128), F32)
            for i in range(S):
                res = lax.dot_general(v_s[g * S + i], w, (((1,), (1,)), ((), ())), preferred_element_type=F32)
                for h in range(8):
                    acc = jnp.where(lane == i * 8 + h, res[64 * h:64 * h + 64], acc)
            return acc

        def finish(g, acc):
            part_s[g] = acc.astype(BF16).reshape(4, 16, 128)

        pltpu.make_async_copy(q_hbm, q_s, q_sem).wait()
        kcopy(0).wait()
        scores(0)
        for g in range(G):
            if g + 1 < G:
                kcopy(g + 1).wait()
            vcopy(g).wait()
            if g + 1 < G:
                scores(g + 1)
            finish(g, values(g))
            if g == 0:
                @pl.when(me >= 2)
                def _():
                    pl.semaphore_wait(barrier, N - 1)

            if g == 2:
                @pl.when(me < 2)
                def _():
                    pl.semaphore_wait(barrier, N - 1)
                    give(0)
                    give(1)

            if g < 2:
                @pl.when(me >= 2)
                def _():
                    give(g)
            else:
                @pl.when(me >= 0)
                def _():
                    give(g)
            if g in (4, 5):
                @pl.when(inner & (core == 0))
                def _():
                    together_one(g - 4)

    pl.run_scoped(attend, pltpu.SemaphoreType.DMA(()), pltpu.SemaphoreType.DMA((G,)), pltpu.SemaphoreType.DMA((G,)))

    @pl.when((core == 1) & (inner | edge))
    def _():
        together_one(0)

        @pl.when(me != 1)
        def _():
            together_one(1)

    @pl.when(edge & (core == 0) | (me == N - 1))
    def _():
        together_two(0)
        together_two(1)

    @pl.when(me == 1)
    def _():
        together_near()

    pair, idle = edge & (core == 0), far & (me != N - 1)

    for which, kib in ((idle, 166), (inner | (me == 1), 276), (me == 9, 268), (me == 15, 372), (pair, 388)):
        @pl.when(which)
        def _():
            wait_sent(kib)

    for which, kib in ((idle, 128), (inner | (me == 9), 120), ((me == 8) | (me == 15), 112), (me == 1, 108), (me == 0, 96)):
        @pl.when(which)
        def _():
            wait_recv(kib, recv_o)

    @pl.when(me == 0)
    def _():
        wait_recv(16, recv_x)


def solution(mesh):
    def step(q, k, v):
        k = jnp.transpose(k, (0, 2, 3, 1)).reshape(32, 512, 512)
        v = jnp.transpose(v, (0, 2, 3, 1)).reshape(32, 512, 512)
        o = pl.pallas_call(
            kernel,
            out_shape=pltpu.VMEM((G, 4, 16, 128), BF16),
            in_specs=[pl.BlockSpec(memory_space=pl.ANY)] * 3,
            out_specs=pl.BlockSpec(memory_space=pltpu.VMEM),
            scratch_shapes=[
                pltpu.VMEM((32, 32, 64), BF16),
                pltpu.VMEM((32, 512, 512), BF16),
                pltpu.VMEM((32, 512, 512), BF16),
                pltpu.VMEM((128, 512), BF16),
                pltpu.VMEM((128, 512), BF16),
                pltpu.VMEM((G, 4, 16, 128), BF16),
                pltpu.VMEM((G, 2, 128), F32),
                pltpu.VMEM((2 * N, 16, 128), BF16),
                pltpu.VMEM((2 * N, 2, 128), F32),
                pltpu.VMEM((2 * N, 2, 16, 128), BF16),
                pltpu.VMEM((N, 4, 16, 128), BF16),
                pltpu.VMEM((N, 2, 128), F32),
                pltpu.VMEM((400, 2, 128), F32),
                pltpu.SemaphoreType.DMA(()),
                pltpu.SemaphoreType.DMA((2,)),
                pltpu.SemaphoreType.DMA(()),
                pltpu.SemaphoreType.DMA(()),
                pltpu.SemaphoreType.DMA(()),
            ],
            compiler_params=pltpu.CompilerParams(vmem_limit_bytes=56 << 20, collective_id=0, has_side_effects=True),
        )(q, k, v)
        return o.reshape(G, 64, 128).transpose(0, 2, 1).reshape(32, 32, 64)

    return jax.shard_map(
        step,
        mesh=mesh,
        in_specs=(P("dp", None, None), P("dp", "sp", None, None), P("dp", "sp", None, None)),
        out_specs=P("dp", None, None),
        check_vma=False,
    )
```

```python
import jax
import jax.numpy as jnp
from jax import lax
from jax.experimental import pallas as pl
from jax.experimental.pallas import tpu as pltpu
from jax.sharding import PartitionSpec as P

MESH = pl.DeviceIdType.MESH
F32, BF16 = jnp.float32, jnp.bfloat16
N = 16
G = 8
S = 4
A = 1


def owners_of(g):
    if g in (2, 3):
        return [(0, 0, 2), (8, 2, 2)]
    if g >= 6:
        return [(1, 0, 1), (9, 1, 1), (15, 2, 2)][g - 6:]
    return [((c // 2 * 4 + 1 + c % 2) * 2 + g // 4, c, 1) for c in range(4)]


def kernel(q_hbm, k_hbm, v_hbm, o_ref, q_s, k_s, v_s, w0_s, w1_s, part_s, stat_s, got_p, got_s, pair_p, near_p, near_s, gauge, sent, recv, recv_o, recv_n):
    me = lax.axis_index("sp")
    y, z, core = me // 8, lax.rem(me, 8) // 2, lax.rem(me, 2)
    inner, edge, far = (z == 1) | (z == 2), z == 0, z == 3
    first = core * 4 + jnp.where(inner, 0, 2)
    quarter, base = jnp.where(me == 9, 1, y * 2 + z // 2), y * 2
    w_s = (w0_s, w1_s)

    def copy(src, dst, to, sem):
        pltpu.make_async_remote_copy(src_ref=src, dst_ref=dst, send_sem=sent, recv_sem=sem, device_id={"sp": to}, device_id_type=MESH).start()

    def give(g):
        r = g % 2
        if g == G - 1:
            @pl.when(me != 1)
            def _():
                copy(part_s.at[g], near_p.at[me], 1, recv_n)
                copy(stat_s.at[g], near_s.at[me], 1, recv_n)

        for to, c, n in owners_of(g):
            @pl.when(me != to)
            def _():
                if n == 1:
                    copy(part_s.at[g, c], got_p.at[r * N + me], to, recv.at[r])
                else:
                    copy(part_s.at[g, pl.ds(c, n)], pair_p.at[r * N + me], to, recv.at[r])
                copy(stat_s.at[g], got_s.at[r * N + me], to, recv.at[r])

    def wait_recv(kib, sem):
        pltpu.make_async_remote_copy(
            src_ref=gauge.at[pl.ds(0, kib)], dst_ref=gauge.at[pl.ds(0, kib)], send_sem=sent, recv_sem=sem,
            device_id={"sp": me}, device_id_type=MESH).wait_recv()

    def wait_sent(kib):
        pltpu.make_async_remote_copy(
            src_ref=gauge.at[pl.ds(0, kib)], dst_ref=gauge.at[pl.ds(0, kib)], send_sem=sent, recv_sem=recv_o,
            device_id={"sp": me}, device_id_type=MESH).wait_send()

    def add_up(tiles, stat, at, n, c):
        highs = [stat[at + j, 0:1] for j in range(n)]
        high = highs[0]
        for h in highs[1:]:
            high = jnp.maximum(high, h)
        seen = [jnp.zeros((16, 128), F32)] * c
        total = jnp.zeros((1, 128), F32)
        for j in range(n):
            scale = jnp.exp(highs[j] - high)
            seen = [seen[i] + tiles(at + j, i).astype(F32) * scale for i in range(c)]
            total = total + stat[at + j, 1:2] * scale
        return seen, total, high

    def together_one(r):
        g = first + r
        wait_recv(5 * (N - 1), recv.at[r])
        got_p[r * N + me] = part_s[g, quarter]
        got_s[r * N + me] = stat_s[g]
        seen, total, _ = add_up(lambda j, i: got_p[j], got_s, r * N, N, 1)
        o_ref[g, quarter] = (seen[0] / total).astype(BF16)
        for d in range(N - 1):
            to = d + jnp.where(d >= me, 1, 0)
            if r == 1 and d < 2:
                @pl.when((g < G - 1) | (to >= 2))
                def _():
                    copy(o_ref.at[g, quarter], o_ref.at[g, quarter], to, recv_o)
            else:
                copy(o_ref.at[g, quarter], o_ref.at[g, quarter], to, recv_o)

    def together_two(r):
        g = first + r
        wait_recv(9 * (N - 1), recv.at[r])
        pair_p[r * N + me] = part_s[g, pl.ds(base, 2)]
        got_s[r * N + me] = stat_s[g]
        seen, total, _ = add_up(lambda j, i: pair_p[j, i], got_s, r * N, N, 2)
        for i in range(2):
            o_ref[g, base + i] = (seen[i] / total).astype(BF16)
        half = o_ref.at[g, pl.ds(base, 2)]
        for d in range(N - 1):
            to = d + jnp.where(d >= me, 1, 0)
            if r == 1 and d < 2:
                @pl.when((g < G - 1) | (to >= 2))
                def _():
                    copy(half, half, to, recv_o)
            else:
                copy(half, half, to, recv_o)

    def together_near():
        g = G - 1
        wait_recv(17 * (N - 1), recv_n)
        near_p[me] = part_s[g]
        near_s[me] = stat_s[g]
        seen, total, _ = add_up(lambda j, i: near_p[j, i], near_s, 0, N, 4)
        for i in range(4):
            o_ref[g, i] = (seen[i] / total).astype(BF16)
        copy(o_ref.at[g], o_ref.at[g], 0, recv_n)
        for to in range(2, N):
            copy(o_ref.at[g, 0], o_ref.at[g, 0], to, recv_o)

    def attend(q_sem, k_sem, v_sem):
        def kcopy(g):
            return pltpu.make_async_copy(k_hbm.at[pl.ds(g * S, S)], k_s.at[pl.ds(g * S, S)], k_sem.at[g])

        def vcopy(g):
            return pltpu.make_async_copy(v_hbm.at[pl.ds(g * S, S)], v_s.at[pl.ds(g * S, S)], v_sem.at[g])

        pltpu.make_async_copy(q_hbm, q_s, q_sem).start()
        kcopy(0).start(priority=1)

        def issue_k(j, _):
            kcopy(j).start(priority=1)
            return 0

        def issue(g, _):
            vcopy(g).start(priority=1)

            @pl.when(g + A + 1 < G)
            def _():
                kcopy(g + A + 1).start(priority=1)

            return 0

        lax.fori_loop(1, A + 1, issue_k, 0)
        lax.fori_loop(0, G, issue, 0)

        barrier = pltpu.get_barrier_semaphore()
        for d in range(1, N):
            pl.semaphore_signal(barrier, inc=1, device_id={"sp": lax.rem(me + d, N)}, device_id_type=MESH)

        lane64 = lax.broadcasted_iota(jnp.int32, (16, 128), 1) // 64
        row4 = lax.broadcasted_iota(jnp.int32, (16, 128), 0) // 4
        lane = lax.broadcasted_iota(jnp.int32, (64, 128), 1) // 4
        rowid = lax.broadcasted_iota(jnp.int32, (16, 128), 0)
        laneid = lax.broadcasted_iota(jnp.int32, (16, 128), 1)

        def scores(g):
            slot = g % 2
            mrow = jnp.zeros((16, 128), F32)
            lrow = jnp.zeros((16, 128), F32)
            for i in range(S):
                qb = q_s[g * S + i].astype(F32)
                qq = jnp.concatenate([qb, qb], -1)
                for t in range(2):
                    piece = qq[16 * t:16 * t + 16]
                    lo = jnp.where(row4 == lane64, piece, 0.0)
                    hi = jnp.where(row4 == lane64 + 2, piece, 0.0)
                    lhs = jnp.concatenate([lo, hi], -1).astype(BF16)
                    s = jnp.dot(lhs, k_s[g * S + i, 256 * t:256 * t + 256, :], preferred_element_type=F32)
                    m = jnp.max(s, -1, keepdims=True)
                    p = jnp.exp((s - m) * 0.125)
                    l = jnp.sum(p, -1, keepdims=True)
                    r = 32 * i + 16 * t
                    w_s[slot][r:r + 16, :] = p.astype(BF16)
                    hit = laneid == rowid + r
                    mrow = jnp.where(hit, m * 0.125, mrow)
                    lrow = jnp.where(hit, l, lrow)
            stat_s[g, 0:1] = jnp.sum(mrow, 0, keepdims=True)
            stat_s[g, 1:2] = jnp.sum(lrow, 0, keepdims=True)

        def values(g):
            w = w_s[g % 2][...]
            acc = jnp.zeros((64, 128), F32)
            for i in range(S):
                res = lax.dot_general(v_s[g * S + i], w, (((1,), (1,)), ((), ())), preferred_element_type=F32)
                for h in range(8):
                    acc = jnp.where(lane == i * 8 + h, res[64 * h:64 * h + 64], acc)
            return acc

        def finish(g, acc):
            part_s[g] = acc.astype(BF16).reshape(4, 16, 128)

        pltpu.make_async_copy(q_hbm, q_s, q_sem).wait()
        kcopy(0).wait()
        scores(0)
        for g in range(G):
            if g + 1 < G:
                kcopy(g + 1).wait()
            vcopy(g).wait()
            if g + 1 < G:
                scores(g + 1)
            finish(g, values(g))
            if g == 0:
                @pl.when(me >= 2)
                def _():
                    pl.semaphore_wait(barrier, N - 1)

            if g == 2:
                @pl.when(me < 2)
                def _():
                    pl.semaphore_wait(barrier, N - 1)
                    give(0)
                    give(1)

            if g < 2:
                @pl.when(me >= 2)
                def _():
                    give(g)
            else:
                @pl.when(me >= 0)
                def _():
                    give(g)
            if g in (4, 5):
                @pl.when(inner & (core == 0))
                def _():
                    together_one(g - 4)

    pl.run_scoped(attend, pltpu.SemaphoreType.DMA(()), pltpu.SemaphoreType.DMA((G,)), pltpu.SemaphoreType.DMA((G,)))

    @pl.when((core == 1) & (inner | edge))
    def _():
        together_one(0)

        @pl.when(me != 1)
        def _():
            together_one(1)

    @pl.when(edge & (core == 0) | (me == N - 1))
    def _():
        together_two(0)
        together_two(1)

    @pl.when(me == 1)
    def _():
        together_near()

    pair, idle = edge & (core == 0), far & (me != N - 1)

    for which, kib in ((idle, 166), (inner | (me == 1), 276), (me == 9, 268), (me == 15, 372), (pair, 388)):
        @pl.when(which)
        def _():
            wait_sent(kib)

    for which, kib in ((idle, 128), (inner | (me == 9), 120), ((me == 8) | (me == 15), 112), (me == 1, 108), (me == 0, 96)):
        @pl.when(which)
        def _():
            wait_recv(kib, recv_o)

    @pl.when(me == 0)
    def _():
        wait_recv(16, recv_n)


def solution(mesh):
    def step(q, k, v):
        k = jnp.transpose(k, (0, 2, 3, 1)).reshape(32, 512, 512)
        v = jnp.transpose(v, (0, 2, 3, 1)).reshape(32, 512, 512)
        o = pl.pallas_call(
            kernel,
            out_shape=pltpu.VMEM((G, 4, 16, 128), BF16),
            in_specs=[pl.BlockSpec(memory_space=pl.ANY)] * 3,
            out_specs=pl.BlockSpec(memory_space=pltpu.VMEM),
            scratch_shapes=[
                pltpu.VMEM((32, 32, 64), BF16),
                pltpu.VMEM((32, 512, 512), BF16),
                pltpu.VMEM((32, 512, 512), BF16),
                pltpu.VMEM((128, 512), BF16),
                pltpu.VMEM((128, 512), BF16),
                pltpu.VMEM((G, 4, 16, 128), BF16),
                pltpu.VMEM((G, 2, 128), F32),
                pltpu.VMEM((2 * N, 16, 128), BF16),
                pltpu.VMEM((2 * N, 2, 128), F32),
                pltpu.VMEM((2 * N, 2, 16, 128), BF16),
                pltpu.VMEM((N, 4, 16, 128), BF16),
                pltpu.VMEM((N, 2, 128), F32),
                pltpu.VMEM((400, 2, 128), F32),
                pltpu.SemaphoreType.DMA(()),
                pltpu.SemaphoreType.DMA((2,)),
                pltpu.SemaphoreType.DMA(()),
                pltpu.SemaphoreType.DMA(()),
            ],
            compiler_params=pltpu.CompilerParams(vmem_limit_bytes=56 << 20, collective_id=0, has_side_effects=True),
        )(q, k, v)
        return o.reshape(G, 64, 128).transpose(0, 2, 1).reshape(32, 32, 64)

    return jax.shard_map(
        step,
        mesh=mesh,
        in_specs=(P("dp", None, None), P("dp", "sp", None, None), P("dp", "sp", None, None)),
        out_specs=P("dp", None, None),
        check_vma=False,
    )
```
